32 devices in a mesh: seq: 8 (over y, x, core), tensor: 4 (over z).
Axes of the slice: x: 2, y: 2, z: 4, core: 2. Of those that a mesh axis runs over, the one named last changes fastest.
Arguments:
- tokens: bfloat16 [5760, 1536], P('seq'), may hold values from -6 to 6
- norm_gain: float32 [1536], replicated, may hold values from 0.1 to 1.9
- w_qkv: bfloat16 [1536, 3, 1536], P(None, None, 'tensor'), may hold values from -8 to 8
- w_out: bfloat16 [1536, 1536], P('tensor'), may hold values from -0.15625 to 0.15625
- post_gain: float32 [1536], replicated, may hold values from 0.1 to 1.9
- w_up: bfloat16 [1536, 6144], P(None, 'tensor'), may hold values from -0.15625 to 0.15625
- w_down: bfloat16 [6144, 1536], P('tensor'), may hold values from -0.078125 to 0.078125
Outputs:
- layer_out: bfloat16 [5760, 1536], P('seq')
The draws below stay inside these ranges and needn't reach their ends.
All inputs are finite; a program needn't handle non-finite values.
Results may differ from the reference program's by a relative error of at most 0.015.
Values may be sent and summed in bfloat16 or wider, within the bound.
A program may use at most 128 MiB of HBM per device.

```python
import math
import jax
import jax.numpy as jnp
from jax import lax

D = 1536
HEADS = 32
HD = 48
FF = 6144
TOK_DEV = 720
TOKENS = 5760
N_TENSOR = 4


def draw_w_qkv(key, part):
    base = jax.random.normal(key, (D, 3, HEADS * HD), jnp.float32) * D ** (-0.5)
    levels = jax.random.uniform(jax.random.fold_in(key, 3), (HEADS,), jnp.float32, math.log(1.5), math.log(3.5))
    sharpness = jnp.repeat(jnp.exp(levels), HD)
    query = base[:, 0, :] * sharpness[None, :]
    stacked = jnp.stack([query, base[:, 1, :], base[:, 2, :]], axis=1)
    return jnp.clip(stacked, -8.0, 8.0).astype(jnp.bfloat16)


def level_of(stream_key, shape, cuts, least, top_value):
    def one(dim, parts):
        steps = jax.random.uniform(jax.random.fold_in(jax.random.fold_in(stream_key, 6), dim), (parts,), jnp.float32, least / len(cuts), top_value / len(cuts))
        return jnp.repeat(jnp.exp(steps), shape[dim] // parts).reshape((-1,) + (1,) * (len(shape) - dim - 1))

    level = one(*cuts[0])
    for cut in cuts[1:]:
        level = level * one(*cut)
    return level


def scatter_about(rng, extent, scale, bound, split=(), dtype=jnp.bfloat16):
    loudness = level_of(rng, extent, split, -0.22, 0.18) if split else 1.0
    array = jax.random.normal(rng, extent, jnp.float32) * scale * loudness
    return jnp.minimum(jnp.maximum(array, -bound), bound).astype(dtype)


def setup_inputs(seed: int = 0) -> dict:
    key_list = jax.random.split(jax.random.key(seed), 8)
    return {
        "tokens": scatter_about(key_list[0], (TOKENS, D), 1.0, 6.0, ((0, 8),)),
        "norm_gain": jnp.clip(1.0 + 0.18 * jax.random.normal(key_list[1], (D,), jnp.float32), 0.1, 1.9),
        "w_qkv": draw_w_qkv(jax.random.fold_in(key_list[7], 71), 0),
        "w_out": scatter_about(key_list[3], (HEADS * HD, D), (HEADS * HD) ** -0.5, 0.15625, ((0, 4),)),
        "post_gain": jnp.clip(1.0 + 0.18 * jax.random.normal(key_list[4], (D,), jnp.float32), 0.1, 1.9),
        "w_up": scatter_about(key_list[5], (D, FF), D ** -0.5, 0.15625, ((1, 4),)),
        "w_down": scatter_about(key_list[6], (FF, D), FF ** -0.5, 0.078125, ((0, 4),)),
    }


def layer_norm(values, gain):
    mean = lax.optimization_barrier(jnp.mean(values, axis=-1, keepdims=True))
    centred = values - mean
    var = lax.optimization_barrier(jnp.mean(centred * centred, axis=-1, keepdims=True))
    return centred * lax.rsqrt(var + 1e-05) * gain

def one_head(operands):
    query, key, value = operands
    scale = 1.0 / HD ** 0.5

    def block(query_block):
        scores = jnp.dot(query_block, key.T, preferred_element_type=jnp.float32) * scale
        peak = lax.optimization_barrier(jnp.max(scores, axis=-1, keepdims=True))
        weights = jnp.exp(scores - peak)
        total = lax.optimization_barrier(jnp.sum(weights, axis=-1, keepdims=True))
        return jnp.dot(weights.astype(jnp.bfloat16), value, preferred_element_type=jnp.float32) / total
    blocks = query.reshape(TOKENS // TOK_DEV, TOK_DEV, HD)
    return lax.map(block, blocks).reshape(TOKENS, HD)

def grouped_sum(left, right):
    width = left.shape[1] // N_TENSOR
    result = jnp.zeros((left.shape[0], right.shape[1]), jnp.float32)
    for group in range(N_TENSOR):
        term = jnp.dot(left[:, group * width:(group + 1) * width], right[group * width:(group + 1) * width], preferred_element_type=jnp.float32)
        term = lax.optimization_barrier(term.astype(jnp.bfloat16))
        result = result + term.astype(jnp.float32)
    return result

def reference(tokens, norm_gain, w_qkv, w_out, post_gain, w_up, w_down):
    base = tokens.astype(jnp.float32)
    normed = layer_norm(base, norm_gain).astype(jnp.bfloat16)
    qkv = jnp.dot(normed, w_qkv.reshape(D, 3 * HEADS * HD), preferred_element_type=jnp.float32).astype(jnp.bfloat16)
    qkv = qkv.reshape(TOKENS, 3, HEADS, HD)
    query = jnp.transpose(qkv[:, 0], (1, 0, 2))
    key = jnp.transpose(qkv[:, 1], (1, 0, 2))
    value = jnp.transpose(qkv[:, 2], (1, 0, 2))
    heads = lax.map(one_head, (query, key, value))
    attended = jnp.transpose(heads, (1, 0, 2)).reshape(TOKENS, HEADS * HD).astype(jnp.bfloat16)
    mixed = base + grouped_sum(attended, w_out)
    post = layer_norm(mixed, post_gain).astype(jnp.bfloat16)
    hidden = jax.nn.gelu(jnp.dot(post, w_up, preferred_element_type=jnp.float32), approximate=True).astype(jnp.bfloat16)
    return (mixed + grouped_sum(hidden, w_down)).astype(jnp.bfloat16)
```

```python
import functools

import jax
import jax.numpy as jnp
from jax import lax
from jax.experimental import pallas as pl
from jax.experimental.pallas import tpu as pltpu
from jax.sharding import PartitionSpec as P

HD = 48
ONES = 16
LOG2E = 1.4426950408889634
MESH = pl.DeviceIdType.MESH
CONTRACT_FIRST = (((0,), (0,)), ((), ()))


def layer_norm(values, gain):
    mean = jnp.mean(values, axis=-1, keepdims=True)
    centred = values - mean
    var = jnp.mean(centred * centred, axis=-1, keepdims=True)
    return centred * lax.rsqrt(var + 1e-05) * gain


def flip(chip, mask, chips):
    result, bit = 0, 1
    while bit < chips:
        mine, other = (chip // bit) % 2, (mask // bit) % 2
        result = result + bit * (mine + other - 2 * mine * other)
        bit *= 2
    return result


def attend_kernel(
    n, lanes, heads, group, q_ref, kv_ref, w_ref, o_ref, wide_ref,
    held, accum, peak, own_sem, send_sem, pass_sem, recv_sem, wsend_sem, wrecv_sem, wpass_sem, wpassed_sem,
):
    seq, lane = lax.axis_index("seq"), lax.axis_index("tensor")
    chips = n // 2
    chip, core = seq // 2, seq % 2
    sibling = chip * 2 + 1 - core
    half = w_ref.shape[0] // 2
    mine = pl.ds(pl.multiple_of(core * half, half), half)
    others = pl.ds(pl.multiple_of((1 - core) * half, half), half)

    def order(step, which):
        if chips < 4:
            return step + 1
        return step + 1 + which * (jnp.where(step == 0, 1, 0) - jnp.where(step == 1, 1, 0))

    def send(source, slot, target, sem):
        return pltpu.make_async_remote_copy(
            src_ref=source,
            dst_ref=held.at[slot],
            send_sem=sem,
            recv_sem=recv_sem.at[slot],
            device_id=(target, lane),
            device_id_type=MESH,
        )

    def spread(step):
        return pltpu.make_async_remote_copy(
            src_ref=w_ref.at[mine],
            dst_ref=wide_ref.at[lane, mine],
            send_sem=wsend_sem.at[step],
            recv_sem=wrecv_sem.at[lane],
            device_id=(seq, (lane + step) % lanes),
            device_id_type=MESH,
        )

    def spread_arrival(source):
        return pltpu.make_async_remote_copy(
            src_ref=w_ref.at[mine],
            dst_ref=wide_ref.at[source, mine],
            send_sem=wsend_sem.at[1],
            recv_sem=wrecv_sem.at[source],
            device_id=(seq, (lane + 1) % lanes),
            device_id_type=MESH,
        )

    def hand(source, part):
        return pltpu.make_async_remote_copy(
            src_ref=wide_ref.at[source, part],
            dst_ref=wide_ref.at[source, part],
            send_sem=wpass_sem.at[source],
            recv_sem=wpassed_sem.at[source],
            device_id=(sibling, lane),
            device_id_type=MESH,
        )

    barrier = pltpu.get_barrier_semaphore()
    pl.semaphore_signal(barrier, inc=1, device_id=(sibling, lane), device_id_type=MESH)
    for step in range(1, chips):
        pl.semaphore_signal(
            barrier, inc=1, device_id=(flip(chip, step, chips) * 2 + core, lane), device_id_type=MESH
        )
    for step in range(1, lanes):
        pl.semaphore_signal(barrier, inc=1, device_id=(seq, (lane + step) % lanes), device_id_type=MESH)
    pl.semaphore_wait(barrier, chips + lanes - 1)

    for step in range(chips - 1):
        target = flip(chip, order(step, core), chips) * 2 + core
        send(kv_ref, seq, target, send_sem.at[step]).start()
    send(kv_ref, seq, sibling, pass_sem.at[chips - 1]).start()
    for step in range(1, lanes):
        spread(step).start()
    own = pltpu.make_async_copy(kv_ref, held.at[seq], own_sem)
    own.start()
    accum[...] = jnp.zeros_like(accum)
    peak[...] = jnp.full_like(peak, -1e30)
    own.wait()

    def attend(slot):
        @pl.loop(0, heads // group)
        def _(index):
            members = [index * group + offset for offset in range(group)]
            scores = [
                lax.dot_general(held[slot, h], q_ref[h], CONTRACT_FIRST, preferred_element_type=jnp.float32)
                for h in members
            ]
            for h, score in zip(members, scores):
                value = held[slot, heads + h]
                value = jnp.concatenate([value, jnp.ones((ONES, value.shape[1]), value.dtype)], axis=0)
                old = peak[h]
                new = jnp.maximum(old, jnp.max(score, axis=0, keepdims=True))
                weights = jnp.exp2(score - new).astype(jnp.bfloat16)
                term = jnp.dot(value, weights, preferred_element_type=jnp.float32)
                accum[h] = accum[h] * jnp.exp2(old - new) + term
                peak[h] = new

    @pl.loop(0, n)
    def _(index):
        step, second = index // 2, index % 2
        which = core + second - 2 * core * second
        mask = jnp.where(step == 0, 0, order(step - 1, which))
        slot = flip(chip, mask, chips) * 2 + which

        @pl.when(index > 0)
        def _():
            send(held.at[slot], slot, sibling, pass_sem.at[0]).wait_recv()

        @pl.when(jnp.logical_and(index > 0, second == 0))
        def _():
            send(held.at[slot], slot, sibling, pass_sem.at[step - 1]).start()

        attend(slot)

    for step in range(1, lanes):
        source = (lane + step) % lanes
        spread_arrival(source).wait_recv()
        hand(source, mine).start()

    for h in range(heads):
        o_ref[h] = (accum[h, :HD] / accum[h, HD : HD + 1]).astype(o_ref.dtype)

    for step in range(chips - 1):
        send(kv_ref, seq, sibling, send_sem.at[step]).wait_send()
    for step in range(chips):
        send(kv_ref, seq, sibling, pass_sem.at[step]).wait_send()
    for step in range(1, lanes):
        source = (lane + step) % lanes
        hand(source, others).wait_recv()
        hand(source, mine).wait_send()
        spread(step).wait_send()


def attention(n, lanes, heads, query, pairs, w_out):
    rows = query.shape[2]
    group = next(size for size in (4, 2, 1) if heads % size == 0)
    vmem = pl.BlockSpec(memory_space=pltpu.VMEM)
    hbm = pl.BlockSpec(memory_space=pl.ANY)
    return pl.pallas_call(
        functools.partial(attend_kernel, n, lanes, heads, group),
        out_shape=(
            jax.ShapeDtypeStruct((heads, HD, rows), jnp.bfloat16),
            jax.ShapeDtypeStruct((lanes,) + w_out.shape, jnp.bfloat16),
        ),
        in_specs=[vmem, vmem, hbm],
        out_specs=(vmem, hbm),
        scratch_shapes=[
            pltpu.VMEM((n, 2 * heads, HD, rows), jnp.bfloat16),
            pltpu.VMEM((heads, HD + ONES, rows), jnp.float32),
            pltpu.VMEM((heads, 1, rows), jnp.float32),
            pltpu.SemaphoreType.DMA,
            pltpu.SemaphoreType.DMA((n // 2,)),
            pltpu.SemaphoreType.DMA((n // 2,)),
            pltpu.SemaphoreType.DMA((n,)),
            pltpu.SemaphoreType.DMA((lanes,)),
            pltpu.SemaphoreType.DMA((lanes,)),
            pltpu.SemaphoreType.DMA((lanes,)),
            pltpu.SemaphoreType.DMA((lanes,)),
        ],
        compiler_params=pltpu.CompilerParams(
            collective_id=0, has_side_effects=True, vmem_limit_bytes=56 * 2**20
        ),
        cost_estimate=pl.CostEstimate(
            flops=4 * n * heads * rows * rows * HD,
            bytes_accessed=6 * heads * HD * rows,
            transcendentals=n * heads * rows * rows,
        ),
    )(query, pairs, w_out)


def tail_kernel(
    lanes, chunk, sub,
    mine_ref, tokens_ref, gain_ref, shard_ref, wide_ref, up_ref, down_ref, o_ref,
    att, wo, wu, wd, mixed, term, inbox, res,
    load_sem, right_sem, left_sem, block_sem, send_sem, in_sem, out_sem, res_sem, store_sem,
):
    seq, lane = lax.axis_index("seq"), lax.axis_index("tensor")
    rows = tokens_ref.shape[0]
    chunks, per = rows // chunk, chunk // sub
    middle = lanes // 2
    on_left = lane < middle
    depth = jnp.where(on_left, lane, lanes - 1 - lane)
    inner = jnp.where(on_left, lane + 1, lane - 1)
    outer = jnp.where(on_left, lane - 1, lane + 1)
    central = depth == middle - 1
    has_left, has_right = lane > 0, lane < lanes - 1

    def when(*conditions):
        return pl.when(functools.reduce(jnp.logical_and, conditions))

    def block(source, index, target, sem):
        span = pl.ds(pl.multiple_of(index * chunk, chunk), chunk)
        return pltpu.make_async_remote_copy(
            src_ref=att.at[source, span],
            dst_ref=att.at[source, span],
            send_sem=sem.at[source, index],
            recv_sem=block_sem.at[source, index],
            device_id=(seq, target),
            device_id_type=MESH,
        )

    def piece(index):
        return pl.ds(pl.multiple_of(index * sub, sub), sub)

    def inward(index, box):
        return pltpu.make_async_remote_copy(
            src_ref=term.at[piece(index)],
            dst_ref=inbox.at[box, piece(index)],
            send_sem=send_sem.at[index],
            recv_sem=in_sem.at[box, index],
            device_id=(seq, inner),
            device_id_type=MESH,
        )

    def outward(index):
        return pltpu.make_async_remote_copy(
            src_ref=res.at[piece(index)],
            dst_ref=res.at[piece(index)],
            send_sem=out_sem.at[index],
            recv_sem=res_sem.at[index],
            device_id=(seq, outer),
            device_id_type=MESH,
        )

    def store(index):
        return pltpu.make_async_copy(res.at[piece(index)], o_ref.at[piece(index)], store_sem.at[index])

    barrier = pltpu.get_barrier_semaphore()
    for present, neighbour in ((has_left, lane - 1), (has_right, lane + 1)):
        @pl.when(present)
        def _():
            pl.semaphore_signal(barrier, inc=1, device_id=(seq, neighbour), device_id_type=MESH)

    own = pltpu.make_async_copy(mine_ref, att.at[lane], load_sem.at[lanes + 2])
    own.start()
    for source in range(lanes):
        @pl.when(lane == source)
        def _():
            pltpu.make_async_copy(shard_ref, wo.at[source], load_sem.at[source]).start()

        @pl.when(lane != source)
        def _():
            pltpu.make_async_copy(wide_ref.at[source], wo.at[source], load_sem.at[source]).start()
    wide_loads = [
        pltpu.make_async_copy(up_ref, wu, load_sem.at[lanes]),
        pltpu.make_async_copy(down_ref, wd, load_sem.at[lanes + 1]),
    ]
    for load in wide_loads:
        load.start()
    own.wait()
    pl.semaphore_wait(barrier, has_left.astype(jnp.int32) + has_right.astype(jnp.int32))

    def gather(step):
        for distance in range(lanes):
            index = step + lanes - 1 - distance
            live = jnp.logical_and(index >= 0, index < chunks)
            if distance == 0:
                @when(live, has_right)
                def _():
                    block(lane, index, lane + 1, right_sem).start()

                @when(live, has_left)
                def _():
                    block(lane, index, lane - 1, left_sem).start()
                continue

            @when(live, lane - distance >= 0)
            def _():
                block(lane - distance, index, lane + 1, right_sem).wait_recv()

            @when(live, lane - distance >= 0, has_right)
            def _():
                block(lane - distance, index, lane + 1, right_sem).start()

            @when(live, lane + distance < lanes)
            def _():
                block(lane + distance, index, lane - 1, left_sem).wait_recv()

            @when(live, lane + distance < lanes, has_left)
            def _():
                block(lane + distance, index, lane - 1, left_sem).start()

    def compute(step):
        span = pl.ds(pl.multiple_of(step * chunk, chunk), chunk)
        total = tokens_ref[span, :].astype(jnp.float32)
        for source in range(lanes):
            total = total + jnp.dot(att[source, span, :], wo[source], preferred_element_type=jnp.float32)
        mixed[span, :] = total
        post = layer_norm(total, gain_ref[...]).astype(jnp.bfloat16)
        hidden = jax.nn.gelu(
            jnp.dot(post, wu[...], preferred_element_type=jnp.float32), approximate=True
        ).astype(jnp.bfloat16)
        term[span, :] = jnp.dot(hidden, wd[...], preferred_element_type=jnp.float32).astype(jnp.bfloat16)

    def reduce_inward(index):
        @pl.when(depth > 0)
        def _():
            inward(index, 0).wait_recv()
            rows_here = piece(index)
            term[rows_here, :] = (
                term[rows_here, :].astype(jnp.float32) + inbox[0, rows_here, :].astype(jnp.float32)
            ).astype(jnp.bfloat16)

        inward(index, jnp.where(central, 1, 0)).start()

    def finish(index):
        inward(index, 1).wait_recv()
        rows_here = piece(index)
        both = term[rows_here, :].astype(jnp.float32) + inbox[1, rows_here, :].astype(jnp.float32)
        res[rows_here, :] = (mixed[rows_here, :] + both).astype(jnp.bfloat16)

        @pl.when(depth > 0)
        def _():
            outward(index).start()

        store(index).start()

    def relay(index):
        outward(index).wait_recv()

        @pl.when(depth > 0)
        def _():
            outward(index).start()

        store(index).start()

    def each(step, body):
        @pl.when(jnp.logical_and(step >= 0, step < chunks))
        def _():
            @pl.loop(0, per)
            def _(offset):
                body(step * per + offset)

    @pl.loop(0, chunks + 2 * lanes - 2)
    def _(turn):
        step = turn - (lanes - 1)
        gather(step)

        @pl.when(step == 0)
        def _():
            for source in range(lanes):
                pltpu.make_async_copy(shard_ref, wo.at[source], load_sem.at[source]).wait()
            for load in wide_loads:
                load.wait()

        @pl.when(jnp.logical_and(step >= 0, step < chunks))
        def _():
            compute(step)

        each(step - depth, reduce_inward)

        @pl.when(central)
        def _():
            each(step - middle, finish)

        @when(jnp.logical_not(central), depth > 0)
        def _():
            each(step - middle - (middle - 1 - depth), relay)

    @when(jnp.logical_not(central), depth == 0)
    def _():
        @pl.loop(0, chunks * per)
        def _(index):
            relay(index)

    @pl.loop(0, chunks)
    def _(index):
        for source in range(lanes):
            @when(lane >= source, has_right)
            def _():
                block(source, index, lane + 1, right_sem).wait_send()

            @when(lane <= source, has_left)
            def _():
                block(source, index, lane - 1, left_sem).wait_send()

    @pl.loop(0, chunks * per)
    def _(index):
        inward(index, 0).wait_send()
        store(index).wait()

        @pl.when(depth > 0)
        def _():
            outward(index).wait_send()


def tail(lanes, attended, tokens, gain, w_out, wide, w_up, w_down):
    rows, width = tokens.shape
    span, hidden = w_out.shape[0], w_up.shape[1]
    sub = max(size for size in (16, 32, 48) if rows % size == 0)
    chunk = max(size for size in (sub, 2 * sub, 3 * sub) if rows % size == 0)
    pieces, chunks = rows // sub, rows // chunk
    vmem = pl.BlockSpec(memory_space=pltpu.VMEM)
    hbm = pl.BlockSpec(memory_space=pl.ANY)
    dma = pltpu.SemaphoreType.DMA
    return pl.pallas_call(
        functools.partial(tail_kernel, lanes, chunk, sub),
        out_shape=jax.ShapeDtypeStruct((rows, width), jnp.bfloat16),
        in_specs=[vmem, vmem, vmem, hbm, hbm, hbm, hbm],
        out_specs=hbm,
        scratch_shapes=[
            pltpu.VMEM((lanes, rows, span), jnp.bfloat16),
            pltpu.VMEM((lanes, span, width), jnp.bfloat16),
            pltpu.VMEM((width, hidden), jnp.bfloat16),
            pltpu.VMEM((hidden, width), jnp.bfloat16),
            pltpu.VMEM((rows, width), jnp.float32),
            pltpu.VMEM((rows, width), jnp.bfloat16),
            pltpu.VMEM((2, rows, width), jnp.bfloat16),
            pltpu.VMEM((rows, width), jnp.bfloat16),
            dma((lanes + 3,)),
            dma((lanes, chunks)),
            dma((lanes, chunks)),
            dma((lanes, chunks)),
            dma((pieces,)),
            dma((2, pieces)),
            dma((pieces,)),
            dma((pieces,)),
            dma((pieces,)),
        ],
        compiler_params=pltpu.CompilerParams(
            collective_id=1, has_side_effects=True, vmem_limit_bytes=58 * 2**20
        ),
        cost_estimate=pl.CostEstimate(
            flops=2 * rows * width * (lanes * span + 2 * hidden),
            bytes_accessed=2 * width * (lanes * span + 2 * hidden),
            transcendentals=rows * hidden,
        ),
    )(attended, tokens, gain, w_out, wide, w_up, w_down)


def per_device(n, lanes, tokens, norm_gain, w_qkv, w_out, post_gain, w_up, w_down):
    rows = tokens.shape[0]
    span = w_qkv.shape[2]
    heads = span // HD
    base = tokens.astype(jnp.float32)
    normed = layer_norm(base, norm_gain).astype(jnp.bfloat16)
    weights = w_qkv.reshape(w_qkv.shape[0], -1)
    qkv = lax.dot_general(weights, normed, (((0,), (1,)), ((), ())), preferred_element_type=jnp.float32)
    query = (qkv[:span] * (LOG2E / HD**0.5)).astype(jnp.bfloat16).reshape(heads, HD, rows)
    pairs = qkv[span:].astype(jnp.bfloat16).reshape(2 * heads, HD, rows)
    attended, wide = attention(n, lanes, heads, query, pairs, w_out)
    attended = attended.reshape(span, rows).T
    return tail(lanes, attended, tokens, post_gain.reshape(1, -1), w_out, wide, w_up, w_down)


def solution(mesh):
    placed = (
        P("seq", None),
        P(),
        P(None, None, "tensor"),
        P("tensor", None),
        P(),
        P(None, "tensor"),
        P("tensor", None),
    )
    return jax.shard_map(
        functools.partial(per_device, mesh.shape["seq"], mesh.shape["tensor"]),
        mesh=mesh,
        in_specs=placed,
        out_specs=P("seq", None),
        check_vma=False,
    )
```

```python
import functools

import jax
import jax.numpy as jnp
from jax import lax
from jax.experimental import pallas as pl
from jax.experimental.pallas import tpu as pltpu
from jax.sharding import PartitionSpec as P

HD = 48
ONES = 16
LOG2E = 1.4426950408889634
MESH = pl.DeviceIdType.MESH
CONTRACT_FIRST = (((0,), (0,)), ((), ()))


def layer_norm(values, gain):
    mean = jnp.mean(values, axis=-1, keepdims=True)
    centred = values - mean
    var = jnp.mean(centred * centred, axis=-1, keepdims=True)
    return centred * lax.rsqrt(var + 1e-05) * gain


def flip(chip, mask, chips):
    result, bit = 0, 1
    while bit < chips:
        mine, other = (chip // bit) % 2, (mask // bit) % 2
        result = result + bit * (mine + other - 2 * mine * other)
        bit *= 2
    return result


def layer_kernel(
    n, lanes, parts, chunk, sub,
    q_ref, kv_ref, tokens_ref, gain_ref, shard_ref, up_ref, down_ref, o_ref,
    held, score_a, score_b, column, accum, peak, att, wo, wu, wd, mixed, term, inbox, res,
    load_sem, recv_sem, send_sem, pass_sem, wide_send, wide_recv, part_send, part_pass, part_recv,
    block_sem, right_sem, left_sem, in_send, in_sem, out_send, out_sem, store_sem,
):
    seq, lane = lax.axis_index("seq"), lax.axis_index("tensor")
    chips = n // 2
    bits = chips.bit_length() - 1
    chip, core = seq // 2, seq % 2
    sibling = chip * 2 + 1 - core
    rows = tokens_ref.shape[0]
    groups = kv_ref.shape[0]
    size = kv_ref.shape[1] // 2
    width = size * HD

    def when(*conditions):
        return pl.when(functools.reduce(jnp.logical_and, conditions))

    def remote(source, target, send, recv, device):
        return pltpu.make_async_remote_copy(
            src_ref=source, dst_ref=target, send_sem=send, recv_sem=recv, device_id=device, device_id_type=MESH
        )

    def slot_of(arrival, which):
        turned = sum((arrival // 2**i) % 2 * 2 ** (bits - 1 - i) for i in range(bits))
        return flip(chip, jnp.where(which == 0, arrival, turned), chips) * 2 + which

    def partner(stage):
        return flip(chip, jnp.where(core == 0, 2**stage, 2 ** (bits - 1 - stage)), chips) * 2 + core

    def exchange(group, arrival, stage):
        slot = slot_of(arrival, core)
        block = held.at[slot, group]
        return remote(
            block, block, send_sem.at[stage, group, arrival], recv_sem.at[slot, group], (partner(stage), lane)
        )

    def hand(group, arrival, which):
        slot = slot_of(arrival, which)
        block = held.at[slot, group]
        return remote(block, block, pass_sem.at[group, arrival], recv_sem.at[slot, group], (sibling, lane))

    part = seq % parts
    extent = shard_ref.shape[0] // parts
    mates = parts // 2
    first = chip // mates * mates

    def rows_of(index):
        return pl.ds(pl.multiple_of(index * extent, extent), extent)

    def wide(source, step):
        strip = wo.at[source, rows_of(part)]
        return remote(strip, strip, wide_send.at[step], wide_recv.at[source], (seq, (lane + step) % lanes))

    def mate(step):
        return first + (chip - first + step) % mates

    def spread(source, step):
        strip = wo.at[source, rows_of(part)]
        return remote(
            strip, strip, part_send.at[source, step], part_recv.at[source, part], (mate(step) * 2 + core, lane)
        )

    def share(source, index):
        strip = wo.at[source, rows_of(index)]
        return remote(strip, strip, part_pass.at[source, index], part_recv.at[source, index], (sibling, lane))

    def block(source, group, target, sem):
        rows_here = pl.ds(pl.multiple_of(group * width, width), width)
        piece_ref = att.at[source, rows_here]
        return remote(piece_ref, piece_ref, sem.at[source, group], block_sem.at[source, group], (seq, target))

    has_left, has_right = lane > 0, lane < lanes - 1

    def relay_blocks(group, distance):
        live = jnp.logical_and(group >= 0, group < groups)
        if distance == 0:
            @when(live, has_right)
            def _():
                block(lane, group, lane + 1, right_sem).start()

            @when(live, has_left)
            def _():
                block(lane, group, lane - 1, left_sem).start()

            return

        @when(live, lane - distance >= 0)
        def _():
            block(lane - distance, group, lane + 1, right_sem).wait_recv()

        @when(live, lane - distance >= 0, has_right)
        def _():
            block(lane - distance, group, lane + 1, right_sem).start()

        @when(live, lane + distance < lanes)
        def _():
            block(lane + distance, group, lane - 1, left_sem).wait_recv()

        @when(live, lane + distance < lanes, has_left)
        def _():
            block(lane + distance, group, lane - 1, left_sem).start()

    def tick_middle(group):
        for distance in range(1, lanes, 2):
            relay_blocks(group - (distance + 1) // 2, distance)

    def tick_end(group):
        for distance in range(0, lanes, 2):
            relay_blocks(group - distance // 2, distance)

    barrier = pltpu.get_barrier_semaphore()
    pl.semaphore_signal(barrier, inc=1, device_id=(sibling, lane), device_id_type=MESH)
    for step in range(1, chips):
        pl.semaphore_signal(
            barrier, inc=1, device_id=(flip(chip, step, chips) * 2 + core, lane), device_id_type=MESH
        )
    for step in range(1, lanes):
        pl.semaphore_signal(barrier, inc=1, device_id=(seq, (lane + step) % lanes), device_id_type=MESH)

    own = pltpu.make_async_copy(kv_ref, held.at[seq], load_sem.at[0])
    own.start()
    own_shard = pltpu.make_async_copy(shard_ref, wo.at[lane], load_sem.at[1])
    own_shard.start()
    loads = [
        pltpu.make_async_copy(up_ref, wu, load_sem.at[2]),
        pltpu.make_async_copy(down_ref, wd, load_sem.at[3]),
    ]
    for load in loads:
        load.start()
    own.wait()
    pl.semaphore_wait(barrier, chips + lanes - 1)

    def open_group(group):
        exchange(group, 0, 0).start()
        hand(group, 0, core).start()

    open_group(0)
    own_shard.wait()
    for step in range(1, lanes):
        wide(lane, step).start()

    def prepare(group, index):
        arrival, second = index // 2, index % 2
        which = core + second - 2 * core * second
        hand(group, arrival, which).wait_recv()

        @pl.when(second == 0)
        def _():
            hand(group, arrival, core).start()
            for stage in range(1, bits):
                @pl.when(arrival < 2**stage)
                def _():
                    exchange(group, arrival, stage).start()

        @when(second == 0, arrival == 1)
        def _():
            for stage in range(1, bits):
                exchange(group, 0, stage).start()

            @pl.when(group + 1 < groups)
            def _():
                open_group(group + 1)

    def score(slot, group, member, target):
        result = lax.dot_general(
            held[slot, group, member], q_ref[group * size + member], CONTRACT_FIRST,
            preferred_element_type=jnp.float32,
        )
        target[...] = result
        return jnp.max(result, axis=0, keepdims=True)

    def attend(slot, group, member, source, top):
        value = held[slot, group, size + member]
        value = jnp.concatenate([value, jnp.ones((ONES, rows), value.dtype)], axis=0)
        old = peak[member]
        new = jnp.maximum(old, top)
        weights = jnp.exp2(source[...] - new).astype(jnp.bfloat16)
        term_here = jnp.dot(value, weights, preferred_element_type=jnp.float32)
        accum[member] = accum[member] * jnp.exp2(old - new) + term_here
        peak[member] = new

    scores = (score_a, score_b)
    column[...] = score(seq, 0, 0, score_a)

    @pl.loop(0, groups)
    def _(group):
        accum[...] = jnp.zeros_like(accum)
        peak[...] = jnp.full_like(peak, -1e30)

        @pl.loop(0, n)
        def _(index):
            def place(position):
                arrival, second = position // 2, position % 2
                return slot_of(arrival, core + second - 2 * core * second)

            @pl.when(index == chips)
            def _():
                tick_middle(group)

            @when(index == 3, group == groups - 1)
            def _():
                for step in range(1, lanes):
                    source = (lane + step) % lanes
                    wide(source, step).wait_recv()
                    share(source, part).start()
                    for other in range(1, mates):
                        spread(source, other).start()

            slot = place(index)
            for member in range(size):
                top = column[...]
                if member < size - 1:
                    below = score(slot, group, member + 1, scores[(member + 1) % 2])
                else:
                    @pl.when(index + 1 < n)
                    def _():
                        prepare(group, index + 1)

                    last = index + 1 == n
                    following = jnp.where(last, seq, place((index + 1) % n))
                    next_group = jnp.minimum(group + jnp.where(last, 1, 0), groups - 1)
                    below = score(following, next_group, 0, scores[(member + 1) % 2])
                attend(slot, group, member, scores[member % 2], top)
                column[...] = below

        for member in range(size):
            rows_here = pl.ds(pl.multiple_of(group * width + member * HD, HD), HD)
            att[lane, rows_here, :] = (accum[member, :HD] / accum[member, HD : HD + 1]).astype(att.dtype)
        tick_end(group)

    for group in range(groups, groups + lanes // 2 + 1):
        tick_middle(group)
        tick_end(group)

    for step in range(1, lanes):
        source = (lane + step) % lanes
        for other in range(1, mates):
            index = (mate(other) * 2 + core) % parts
            share(source, index).wait_recv()
            share(source, index).start()
    for step in range(1, lanes):
        source = (lane + step) % lanes
        for other in range(mates):
            share(source, (mate(other) * 2 + 1 - core) % parts).wait_recv()
    for load in loads:
        load.wait()

    full, rest = rows // chunk, rows % chunk
    chunks, per, pieces = full + (rest > 0), chunk // sub, rows // sub
    middle = lanes // 2
    on_left = lane < middle
    depth = jnp.where(on_left, lane, lanes - 1 - lane)
    inner = jnp.where(on_left, lane + 1, lane - 1)
    outer = jnp.where(on_left, lane - 1, lane + 1)
    central = depth == middle - 1

    def piece(index):
        return pl.ds(pl.multiple_of(index * sub, sub), sub)

    def inward(index, box):
        return remote(
            term.at[piece(index)], inbox.at[box, piece(index)],
            in_send.at[index], in_sem.at[box, index], (seq, inner),
        )

    def outward(index):
        return remote(
            res.at[piece(index)], res.at[piece(index)], out_send.at[index], out_sem.at[index], (seq, outer)
        )

    def store(index):
        return pltpu.make_async_copy(res.at[piece(index)], o_ref.at[piece(index)], store_sem.at[index])

    def compute(start, count):
        span = pl.ds(start, count)
        attended = att[:, :, span].reshape(-1, count)
        total = tokens_ref[span, :].astype(jnp.float32) + lax.dot_general(
            attended, wo[...].reshape(-1, wo.shape[2]), CONTRACT_FIRST, preferred_element_type=jnp.float32
        )
        mixed[span, :] = total
        post = layer_norm(total, gain_ref[...]).astype(jnp.bfloat16)
        hidden = jax.nn.gelu(
            jnp.dot(post, wu[...], preferred_element_type=jnp.float32), approximate=True
        ).astype(jnp.bfloat16)
        term[span, :] = jnp.dot(hidden, wd[...], preferred_element_type=jnp.float32).astype(jnp.bfloat16)

    def reduce_inward(index):
        @pl.when(depth > 0)
        def _():
            inward(index, 0).wait_recv()
            rows_here = piece(index)
            term[rows_here, :] = (
                term[rows_here, :].astype(jnp.float32) + inbox[0, rows_here, :].astype(jnp.float32)
            ).astype(jnp.bfloat16)

        inward(index, jnp.where(central, 1, 0)).start()

    def finish(index):
        inward(index, 1).wait_recv()
        rows_here = piece(index)
        both = term[rows_here, :].astype(jnp.float32) + inbox[1, rows_here, :].astype(jnp.float32)
        res[rows_here, :] = (mixed[rows_here, :] + both).astype(jnp.bfloat16)

        @pl.when(depth > 0)
        def _():
            outward(index).start()

        store(index).start()

    def relay(index):
        outward(index).wait_recv()

        @pl.when(depth > 0)
        def _():
            outward(index).start()

        store(index).start()

    def each(step, body):
        @pl.when(jnp.logical_and(step >= 0, step < chunks))
        def _():
            @pl.loop(step * per, jnp.minimum(step * per + per, pieces))
            def _(index):
                body(index)

    @pl.loop(0, chunks + lanes - 1)
    def _(step):
        @pl.when(step < full)
        def _():
            compute(pl.multiple_of(step * chunk, chunk), chunk)

        if rest:
            @pl.when(step == full)
            def _():
                compute(full * chunk, rest)

        each(step - depth, reduce_inward)

        @pl.when(central)
        def _():
            each(step - middle, finish)

        @when(jnp.logical_not(central), depth > 0)
        def _():
            each(step - middle - (middle - 1 - depth), relay)

    @when(jnp.logical_not(central), depth == 0)
    def _():
        @pl.loop(0, pieces)
        def _(index):
            relay(index)

    @pl.loop(0, groups)
    def _(group):
        for source in range(lanes):
            @when(lane >= source, has_right)
            def _():
                block(source, group, lane + 1, right_sem).wait_send()

            @when(lane <= source, has_left)
            def _():
                block(source, group, lane - 1, left_sem).wait_send()

        for arrival in range(chips):
            hand(group, arrival, core).wait_send()
            for stage in range(bits):
                if arrival < 2**stage:
                    exchange(group, arrival, stage).wait_send()

    for step in range(1, lanes):
        wide(lane, step).wait_send()
        source = (lane + step) % lanes
        share(source, part).wait_send()
        for other in range(1, mates):
            spread(source, other).wait_send()
            share(source, (mate(other) * 2 + core) % parts).wait_send()

    @pl.loop(0, pieces)
    def _(index):
        inward(index, 0).wait_send()
        store(index).wait()

        @pl.when(depth > 0)
        def _():
            outward(index).wait_send()


def fused(n, lanes, query, pairs, tokens, gain, w_out, w_up, w_down):
    rows, width = tokens.shape
    span, hidden = w_out.shape[0], w_up.shape[1]
    heads = span // HD
    groups, size = pairs.shape[0], pairs.shape[1] // 2
    parts = n
    while span // parts % 16 or span % parts:
        parts //= 2
    chips = n // 2
    bits = chips.bit_length() - 1
    chunk, sub = 128, 16
    pieces = rows // sub
    vmem = pl.BlockSpec(memory_space=pltpu.VMEM)
    hbm = pl.BlockSpec(memory_space=pl.ANY)
    dma = pltpu.SemaphoreType.DMA
    return pl.pallas_call(
        functools.partial(layer_kernel, n, lanes, parts, chunk, sub),
        out_shape=jax.ShapeDtypeStruct((rows, width), jnp.bfloat16),
        in_specs=[vmem, vmem, vmem, vmem, hbm, hbm, hbm],
        out_specs=hbm,
        scratch_shapes=[
            pltpu.VMEM((n, groups, 2 * size, HD, rows), jnp.bfloat16),
            pltpu.VMEM((rows, rows), jnp.float32),
            pltpu.VMEM((rows, rows), jnp.float32),
            pltpu.VMEM((1, rows), jnp.float32),
            pltpu.VMEM((size, HD + ONES, rows), jnp.float32),
            pltpu.VMEM((size, 1, rows), jnp.float32),
            pltpu.VMEM((lanes, span, rows), jnp.bfloat16),
            pltpu.VMEM((lanes, span, width), jnp.bfloat16),
            pltpu.VMEM((width, hidden), jnp.bfloat16),
            pltpu.VMEM((hidden, width), jnp.bfloat16),
            pltpu.VMEM((rows, width), jnp.float32),
            pltpu.VMEM((rows, width), jnp.bfloat16),
            pltpu.VMEM((2, rows, width), jnp.bfloat16),
            pltpu.VMEM((rows, width), jnp.bfloat16),
            dma((4,)),
            dma((n, groups)),
            dma((bits, groups, chips)),
            dma((groups, chips)),
            dma((lanes,)),
            dma((lanes,)),
            dma((lanes, parts // 2)),
            dma((lanes, parts)),
            dma((lanes, parts)),
            dma((lanes, groups)),
            dma((lanes, groups)),
            dma((lanes, groups)),
            dma((pieces,)),
            dma((2, pieces)),
            dma((pieces,)),
            dma((pieces,)),
            dma((pieces,)),
        ],
        compiler_params=pltpu.CompilerParams(
            collective_id=0, has_side_effects=True, vmem_limit_bytes=63 * 2**20
        ),
        cost_estimate=pl.CostEstimate(
            flops=4 * n * heads * rows * rows * HD + 2 * rows * width * (lanes * span + 2 * hidden),
            bytes_accessed=2 * width * (lanes * span + 2 * hidden),
            transcendentals=n * heads * rows * rows,
        ),
    )(query, pairs, tokens, gain, w_out, w_up, w_down)


def per_device(n, lanes, tokens, norm_gain, w_qkv, w_out, post_gain, w_up, w_down):
    rows = tokens.shape[0]
    span = w_qkv.shape[2]
    heads = span // HD
    base = tokens.astype(jnp.float32)
    normed = layer_norm(base, norm_gain).astype(jnp.bfloat16)
    weights = w_qkv.reshape(w_qkv.shape[0], -1)
    qkv = lax.dot_general(weights, normed, (((0,), (1,)), ((), ())), preferred_element_type=jnp.float32)
    query = (qkv[:span] * (LOG2E / HD**0.5)).astype(jnp.bfloat16).reshape(heads, HD, rows)
    pairs = qkv[span:].astype(jnp.bfloat16).reshape(2, heads // 2, 2, HD, rows)
    pairs = pairs.transpose(1, 0, 2, 3, 4).reshape(heads // 2, 4, HD, rows)
    return fused(n, lanes, query, pairs, tokens, post_gain.reshape(1, -1), w_out, w_up, w_down)


def solution(mesh):
    placed = (
        P("seq", None),
        P(),
        P(None, None, "tensor"),
        P("tensor", None),
        P(),
        P(None, "tensor"),
        P("tensor", None),
    )
    return jax.shard_map(
        functools.partial(per_device, mesh.shape["seq"], mesh.shape["tensor"]),
        mesh=mesh,
        in_specs=placed,
        out_specs=P("seq", None),
        check_vma=False,
    )
```

```python
import functools

import jax
import jax.numpy as jnp
from jax import lax
from jax.experimental import pallas as pl
from jax.experimental.pallas import tpu as pltpu
from jax.sharding import PartitionSpec as P

HD = 48
ONES = 16
LOG2E = 1.4426950408889634
MESH = pl.DeviceIdType.MESH
CONTRACT_FIRST = (((0,), (0,)), ((), ()))


def layer_norm(values, gain):
    mean = jnp.mean(values, axis=-1, keepdims=True)
    centred = values - mean
    var = jnp.mean(centred * centred, axis=-1, keepdims=True)
    return centred * lax.rsqrt(var + 1e-05) * gain


def flip(chip, mask, chips):
    result, bit = 0, 1
    while bit < chips:
        mine, other = (chip // bit) % 2, (mask // bit) % 2
        result = result + bit * (mine + other - 2 * mine * other)
        bit *= 2
    return result


def layer_kernel(
    n, lanes, parts, chunk, sub,
    groups, size, tokens_ref, first_gain_ref, qkv_ref, gain_ref, shard_ref, up_ref, down_ref, o_ref,
    query, wq, held, score_a, score_b, column, accum, peak, att, wo, wu, wd, mixed, term, inbox, res,
    load_sem, recv_sem, send_sem, pass_sem, wide_send, wide_recv, part_send, part_pass, part_recv,
    block_sem, block_send, relay_send, in_send, in_sem, out_send, out_sem, store_sem,
):
    seq, lane = lax.axis_index("seq"), lax.axis_index("tensor")
    chips = n // 2
    bits = chips.bit_length() - 1
    chip, core = seq // 2, seq % 2
    sibling = chip * 2 + 1 - core
    rows = tokens_ref.shape[0]
    width = size * HD

    def when(*conditions):
        return pl.when(functools.reduce(jnp.logical_and, conditions))

    def remote(source, target, send, recv, device):
        return pltpu.make_async_remote_copy(
            src_ref=source, dst_ref=target, send_sem=send, recv_sem=recv, device_id=device, device_id_type=MESH
        )

    def slot_of(arrival, which):
        turned = sum((arrival // 2**i) % 2 * 2 ** (bits - 1 - i) for i in range(bits))
        return flip(chip, jnp.where(which == 0, arrival, turned), chips) * 2 + which

    def partner(stage):
        return flip(chip, jnp.where(core == 0, 2**stage, 2 ** (bits - 1 - stage)), chips) * 2 + core

    def exchange(group, arrival, stage):
        slot = slot_of(arrival, core)
        block = held.at[slot, group]
        return remote(
            block, block, send_sem.at[stage, group, arrival], recv_sem.at[slot, group], (partner(stage), lane)
        )

    def hand(group, arrival, which):
        slot = slot_of(arrival, which)
        block = held.at[slot, group]
        return remote(block, block, pass_sem.at[group, arrival], recv_sem.at[slot, group], (sibling, lane))

    part = seq % parts
    extent = shard_ref.shape[0] // parts
    mates = parts // 2
    first = chip // mates * mates

    def rows_of(index):
        return pl.ds(pl.multiple_of(index * extent, extent), extent)

    def wide(source, step):
        strip = wo.at[source, rows_of(part)]
        return remote(strip, strip, wide_send.at[step], wide_recv.at[source], (seq, (lane + step) % lanes))

    def mate(step):
        return first + (chip - first + step) % mates

    def spread(source, step):
        strip = wo.at[source, rows_of(part)]
        return remote(
            strip, strip, part_send.at[source, step], part_recv.at[source, part], (mate(step) * 2 + core, lane)
        )

    def share(source, index):
        strip = wo.at[source, rows_of(index)]
        return remote(strip, strip, part_pass.at[source, index], part_recv.at[source, index], (sibling, lane))

    def block(source, group, distance):
        rows_here = pl.ds(pl.multiple_of(group * width, width), width)
        strip = att.at[source, rows_here]
        return remote(
            strip, strip, block_send.at[distance + lanes, group], block_sem.at[source, group], (seq, lane + distance)
        )

    def inside(distance):
        return jnp.logical_and(lane + distance >= 0, lane + distance < lanes)

    def onward(group, action):
        for distance in range(2, lanes - 1):
            for sign in (1, -1):
                @when(inside(-sign * distance), inside(sign))
                def _():
                    copy = remote(
                        att.at[lane - sign * distance, pl.ds(pl.multiple_of(group * width, width), width)],
                        att.at[lane - sign * distance, pl.ds(pl.multiple_of(group * width, width), width)],
                        relay_send.at[sign * distance + lanes, group],
                        block_sem.at[lane - sign * distance, group],
                        (seq, lane + sign),
                    )
                    if action:
                        copy.wait_recv()
                        copy.start()
                    else:
                        copy.wait_send()

    barrier = pltpu.get_barrier_semaphore()
    pl.semaphore_signal(barrier, inc=1, device_id=(sibling, lane), device_id_type=MESH)
    for step in range(1, chips):
        pl.semaphore_signal(
            barrier, inc=1, device_id=(flip(chip, step, chips) * 2 + core, lane), device_id_type=MESH
        )
    for step in range(1, lanes):
        pl.semaphore_signal(barrier, inc=1, device_id=(seq, (lane + step) % lanes), device_id_type=MESH)

    own = pltpu.make_async_copy(qkv_ref, wq, load_sem.at[0])
    own.start()
    own_shard = pltpu.make_async_copy(shard_ref, wo.at[lane], load_sem.at[1])
    own_shard.start()
    loads = [
        pltpu.make_async_copy(up_ref, wu, load_sem.at[2]),
        pltpu.make_async_copy(down_ref, wd, load_sem.at[3]),
    ]
    for load in loads:
        load.start()
    normed = term

    @pl.loop(0, rows // sub)
    def _(index):
        span = pl.ds(pl.multiple_of(index * sub, sub), sub)
        normed[span, :] = layer_norm(tokens_ref[span, :].astype(jnp.float32), first_gain_ref[...]).astype(normed.dtype)

    pl.semaphore_wait(barrier, chips + lanes - 1)
    own_shard.wait()
    for step in range(1, lanes):
        wide(lane, step).start()
    own.wait()

    def project(which):
        return lax.dot_general(
            wq[which], normed[...], (((0,), (1,)), ((), ())), preferred_element_type=jnp.float32
        )

    for which in (1, 2):
        result = project(which).astype(jnp.bfloat16)
        for group in range(groups):
            strip = result[group * width : (group + 1) * width]
            held[seq, group, (which - 1) * size : which * size] = strip.reshape(size, HD, rows)

    def open_group(group):
        exchange(group, 0, 0).start()
        hand(group, 0, core).start()

    for group in range(groups):
        open_group(group)
    query[...] = (project(0) * (LOG2E / HD**0.5)).astype(jnp.bfloat16).reshape(query.shape)

    def early(group):
        hand(group, 1, core).wait_recv()
        hand(group, 1, core).start()
        for stage in range(1, bits):
            exchange(group, 1, stage).start()

        @pl.when(group + 1 < groups)
        def _():
            for stage in range(1, bits):
                exchange(group + 1, 0, stage).start()

    def prepare(group, index):
        arrival, second = index // 2, index % 2
        which = core + second - 2 * core * second

        @pl.when(index != 2)
        def _():
            hand(group, arrival, which).wait_recv()

        @when(second == 0, arrival > 1)
        def _():
            hand(group, arrival, core).start()
            for stage in range(2, bits):
                @pl.when(arrival < 2**stage)
                def _():
                    exchange(group, arrival, stage).start()

    def score(slot, group, member, target):
        result = lax.dot_general(
            held[slot, group, member], query[group * size + member], CONTRACT_FIRST,
            preferred_element_type=jnp.float32,
        )
        target[...] = result
        return jnp.max(result, axis=0, keepdims=True)

    def attend(slot, group, member, source, top):
        value = held[slot, group, size + member]
        head = group * size + member
        value = jnp.concatenate([value, jnp.ones((ONES, rows), value.dtype)], axis=0)
        old = peak[head]
        new = jnp.maximum(old, top)
        weights = jnp.exp2(source[...] - new).astype(jnp.bfloat16)
        term_here = jnp.dot(value, weights, preferred_element_type=jnp.float32)
        accum[head] = accum[head] * jnp.exp2(old - new) + term_here
        peak[head] = new

    scores = (score_a, score_b)
    column[...] = score(seq, 0, 0, score_a)

    accum[...] = jnp.zeros_like(accum)
    peak[...] = jnp.full_like(peak, -1e30)
    local, total_turns = 2 * groups, n * groups

    def locate(turn):
        later = turn - local
        group = jnp.where(turn < local, turn // 2, later // (n - 2))
        index = jnp.where(turn < local, turn % 2, 2 + later % (n - 2))
        arrival, second = index // 2, index % 2
        return group, index, slot_of(arrival, core + second - 2 * core * second)

    @pl.loop(0, total_turns)
    def _(turn):
        group, index, slot = locate(turn)

        @pl.when(turn == min(2, local - 1))
        def _():
            for stage in range(1, bits):
                exchange(0, 0, stage).start()

        @pl.when(turn == min(4, local - 1))
        def _():
            early(0)

        @when(index == 3, group + 1 < groups)
        def _():
            early(group + 1)

        @when(index == 4, group == max(groups - 2, 0))
        def _():
            for step in range(1, lanes):
                source = (lane + step) % lanes
                wide(source, step).wait_recv()
                share(source, part).start()
                for other in range(1, mates):
                    spread(source, other).start()

        for member in range(size):
            top = column[...]
            if member < size - 1:
                below = score(slot, group, member + 1, scores[(member + 1) % 2])
            else:
                next_group, next_index, next_slot = locate(jnp.minimum(turn + 1, total_turns - 1))

                @when(turn + 1 < total_turns, next_index > 0)
                def _():
                    prepare(next_group, next_index)

                below = score(next_slot, next_group, 0, scores[(member + 1) % 2])
            attend(slot, group, member, scores[member % 2], top)
            column[...] = below

        @pl.when(index == n - 1)
        def _():
            for member in range(size):
                head = group * size + member
                rows_here = pl.ds(pl.multiple_of(head * HD, HD), HD)
                att[lane, rows_here, :] = (accum[head, :HD] / accum[head, HD : HD + 1]).astype(att.dtype)
            for distance in (1, -1, 2, -2):
                @pl.when(inside(distance))
                def _():
                    block(lane, group, distance).start()

            @pl.when(group > 0)
            def _():
                onward(group - 1, True)

    onward(groups - 1, True)

    for step in range(1, lanes):
        source = (lane + step) % lanes
        for other in range(1, mates):
            index = (mate(other) * 2 + core) % parts
            share(source, index).wait_recv()
            share(source, index).start()
    for step in range(1, lanes):
        source = (lane + step) % lanes
        for other in range(mates):
            share(source, (mate(other) * 2 + 1 - core) % parts).wait_recv()
    for group in range(groups):
        for distance in (1, 2, *range(3, lanes)):
            for sign in (1, -1):
                if distance < 2 or distance == lanes - 1:
                    arrived = inside(sign * distance)
                else:
                    arrived = jnp.logical_and(inside(sign * distance), jnp.logical_not(inside(-sign)))

                @pl.when(arrived)
                def _():
                    block(lane + sign * distance, group, 1).wait_recv()
    for load in loads:
        load.wait()

    full, rest = rows // chunk, rows % chunk
    chunks, pieces = full + (rest > 0), rows // sub
    middle = lanes // 2
    on_left = lane < middle
    depth = jnp.where(on_left, lane, lanes - 1 - lane)
    inner = jnp.where(on_left, lane + 1, lane - 1)
    outer = jnp.where(on_left, lane - 1, lane + 1)
    central = depth == middle - 1

    def piece(index):
        return pl.ds(pl.multiple_of(index * sub, sub), sub)

    def inward(index, box):
        return remote(
            term.at[piece(index)], inbox.at[box, piece(index)],
            in_send.at[index], in_sem.at[box, index], (seq, inner),
        )

    def outward(index):
        return remote(
            res.at[piece(index)], res.at[piece(index)], out_send.at[index], out_sem.at[index], (seq, outer)
        )

    def store(index):
        return pltpu.make_async_copy(res.at[piece(index)], o_ref.at[piece(index)], store_sem.at[index])

    def compute(start, count):
        span = pl.ds(start, count)
        attended = att[:, :, span].reshape(-1, count)
        total = tokens_ref[span, :].astype(jnp.float32) + lax.dot_general(
            attended, wo[...].reshape(-1, wo.shape[2]), CONTRACT_FIRST, preferred_element_type=jnp.float32
        )
        mixed[span, :] = total
        post = layer_norm(total, gain_ref[...]).astype(jnp.bfloat16)
        hidden = jax.nn.gelu(
            jnp.dot(post, wu[...], preferred_element_type=jnp.float32), approximate=True
        ).astype(jnp.bfloat16)
        term[span, :] = jnp.dot(hidden, wd[...], preferred_element_type=jnp.float32).astype(jnp.bfloat16)

    def reduce_inward(index):
        @pl.when(depth > 0)
        def _():
            inward(index, 0).wait_recv()
            rows_here = piece(index)
            term[rows_here, :] = (
                term[rows_here, :].astype(jnp.float32) + inbox[0, rows_here, :].astype(jnp.float32)
            ).astype(jnp.bfloat16)

        inward(index, jnp.where(central, 1, 0)).start()

    def finish(index):
        inward(index, 1).wait_recv()
        rows_here = piece(index)
        both = term[rows_here, :].astype(jnp.float32) + inbox[1, rows_here, :].astype(jnp.float32)
        res[rows_here, :] = (mixed[rows_here, :] + both).astype(jnp.bfloat16)

        @pl.when(depth > 0)
        def _():
            outward(index).start()

        store(index).start()

    def relay(index):
        outward(index).wait_recv()

        @pl.when(depth > 0)
        def _():
            outward(index).start()

        store(index).start()

    lag = 2

    @pl.loop(0, chunks + middle - 1)
    def _(step):
        @pl.when(step < full)
        def _():
            compute(pl.multiple_of(step * chunk, chunk), chunk)

        if rest:
            @pl.when(step == full)
            def _():
                compute(full * chunk, rest)

        behind = step - depth

        @when(behind >= 0, behind < chunks)
        def _():
            @pl.loop(behind * chunk // sub, jnp.minimum(behind * chunk + chunk, rows) // sub)
            def _(index):
                reduce_inward(index)

                @when(central, index >= lag)
                def _():
                    finish(index - lag)

    @pl.when(central)
    def _():
        for index in range(pieces - lag, pieces):
            finish(index)

    @pl.when(jnp.logical_not(central))
    def _():
        @pl.loop(0, pieces)
        def _(index):
            relay(index)

    @pl.loop(0, groups)
    def _(group):
        for distance in (1, -1, 2, -2):
            @pl.when(inside(distance))
            def _():
                block(lane, group, distance).wait_send()

        onward(group, False)


        for arrival in range(chips):
            hand(group, arrival, core).wait_send()
            for stage in range(bits):
                if arrival < 2**stage:
                    exchange(group, arrival, stage).wait_send()

    for step in range(1, lanes):
        wide(lane, step).wait_send()
        source = (lane + step) % lanes
        share(source, part).wait_send()
        for other in range(1, mates):
            spread(source, other).wait_send()
            share(source, (mate(other) * 2 + core) % parts).wait_send()

    @pl.loop(0, pieces)
    def _(index):
        inward(index, 0).wait_send()
        store(index).wait()

        @pl.when(depth > 0)
        def _():
            outward(index).wait_send()


def fused(n, lanes, tokens, first_gain, w_qkv, gain, w_out, w_up, w_down):
    rows, width = tokens.shape
    span, hidden = w_out.shape[0], w_up.shape[1]
    heads = span // HD
    size = 2
    groups = heads // size
    parts = n
    while span // parts % 16 or span % parts:
        parts //= 2
    chips = n // 2
    bits = chips.bit_length() - 1
    chunk = 128
    sub = max(size for size in (16, 32, 48) if rows % size == 0)
    pieces = rows // sub
    vmem = pl.BlockSpec(memory_space=pltpu.VMEM)
    hbm = pl.BlockSpec(memory_space=pl.ANY)
    dma = pltpu.SemaphoreType.DMA
    return pl.pallas_call(
        functools.partial(layer_kernel, n, lanes, parts, chunk, sub, groups, size),
        out_shape=jax.ShapeDtypeStruct((rows, width), jnp.bfloat16),
        in_specs=[vmem, vmem, hbm, vmem, hbm, hbm, hbm],
        out_specs=hbm,
        scratch_shapes=[
            pltpu.VMEM((heads, HD, rows), jnp.bfloat16),
            pltpu.VMEM(w_qkv.shape, jnp.bfloat16),
            pltpu.VMEM((n, groups, 2 * size, HD, rows), jnp.bfloat16),
            pltpu.VMEM((rows, rows), jnp.float32),
            pltpu.VMEM((rows, rows), jnp.float32),
            pltpu.VMEM((1, rows), jnp.float32),
            pltpu.VMEM((heads, HD + ONES, rows), jnp.float32),
            pltpu.VMEM((heads, 1, rows), jnp.float32),
            pltpu.VMEM((lanes, span, rows), jnp.bfloat16),
            pltpu.VMEM((lanes, span, width), jnp.bfloat16),
            pltpu.VMEM((width, hidden), jnp.bfloat16),
            pltpu.VMEM((hidden, width), jnp.bfloat16),
            pltpu.VMEM((rows, width), jnp.float32),
            pltpu.VMEM((rows, width), jnp.bfloat16),
            pltpu.VMEM((2, rows, width), jnp.bfloat16),
            pltpu.VMEM((rows, width), jnp.bfloat16),
            dma((4,)),
            dma((n, groups)),
            dma((bits, groups, chips)),
            dma((groups, chips)),
            dma((lanes,)),
            dma((lanes,)),
            dma((lanes, parts // 2)),
            dma((lanes, parts)),
            dma((lanes, parts)),
            dma((lanes, groups)),
            dma((2 * lanes, groups)),
            dma((2 * lanes, groups)),
            dma((pieces,)),
            dma((2, pieces)),
            dma((pieces,)),
            dma((pieces,)),
            dma((pieces,)),
        ],
        compiler_params=pltpu.CompilerParams(
            collective_id=0, has_side_effects=True, vmem_limit_bytes=63 * 2**20
        ),
        cost_estimate=pl.CostEstimate(
            flops=4 * n * heads * rows * rows * HD + 2 * rows * width * (lanes * span + 2 * hidden),
            bytes_accessed=2 * width * (lanes * span + 2 * hidden),
            transcendentals=n * heads * rows * rows,
        ),
    )(tokens, first_gain, w_qkv, gain, w_out, w_up, w_down)


def per_device(n, lanes, tokens, norm_gain, w_qkv, w_out, post_gain, w_up, w_down):
    w_qkv = w_qkv.transpose(1, 0, 2)
    return fused(n, lanes, tokens, norm_gain, w_qkv, post_gain, w_out, w_up, w_down)


def solution(mesh):
    placed = (
        P("seq", None),
        P(),
        P(None, None, "tensor"),
        P("tensor", None),
        P(),
        P(None, "tensor"),
        P("tensor", None),
    )
    return jax.shard_map(
        functools.partial(per_device, mesh.shape["seq"], mesh.shape["tensor"]),
        mesh=mesh,
        in_specs=placed,
        out_specs=P("seq", None),
        check_vma=False,
    )
```

```python
import functools

import jax
import jax.numpy as jnp
from jax import lax
from jax.experimental import pallas as pl
from jax.experimental.pallas import tpu as pltpu
from jax.sharding import PartitionSpec as P

HD = 48
ONES = 16
LOG2E = 1.4426950408889634
MESH = pl.DeviceIdType.MESH
CONTRACT_FIRST = (((0,), (0,)), ((), ()))


def layer_norm(values, gain):
    mean = jnp.mean(values, axis=-1, keepdims=True)
    centred = values - mean
    var = jnp.mean(centred * centred, axis=-1, keepdims=True)
    return centred * lax.rsqrt(var + 1e-05) * gain


def flip(chip, mask, chips):
    result, bit = 0, 1
    while bit < chips:
        mine, other = (chip // bit) % 2, (mask // bit) % 2
        result = result + bit * (mine + other - 2 * mine * other)
        bit *= 2
    return result


def layer_kernel(
    n, lanes, parts, chunk, sub,
    groups, size, tokens_ref, first_gain_ref, qkv_ref, gain_ref, shard_ref, up_ref, down_ref, o_ref,
    query, wq, held, score_a, score_b, column, accum, peak, att, wo, wu, wd, mixed, term, inbox, res,
    load_sem, recv_sem, send_sem, pass_sem, wide_send, wide_recv, part_send, part_pass, part_recv,
    block_sem, block_send, relay_send, in_send, in_sem, out_send, out_sem, store_sem,
):
    seq, lane = lax.axis_index("seq"), lax.axis_index("tensor")
    chips = n // 2
    bits = chips.bit_length() - 1
    chip, core = seq // 2, seq % 2
    sibling = chip * 2 + 1 - core
    rows = tokens_ref.shape[0]
    width = size * HD

    def when(*conditions):
        return pl.when(functools.reduce(jnp.logical_and, conditions))

    def remote(source, target, send, recv, device):
        return pltpu.make_async_remote_copy(
            src_ref=source, dst_ref=target, send_sem=send, recv_sem=recv, device_id=device, device_id_type=MESH
        )

    def slot_of(arrival, which):
        turned = sum((arrival // 2**i) % 2 * 2 ** (bits - 1 - i) for i in range(bits))
        return flip(chip, jnp.where(which == 0, arrival, turned), chips) * 2 + which

    def partner(stage):
        return flip(chip, jnp.where(core == 0, 2**stage, 2 ** (bits - 1 - stage)), chips) * 2 + core

    def exchange(group, arrival, stage):
        slot = slot_of(arrival, core)
        block = held.at[slot, group]
        return remote(
            block, block, send_sem.at[stage, group, arrival], recv_sem.at[slot, group], (partner(stage), lane)
        )

    def hand(group, arrival, which):
        slot = slot_of(arrival, which)
        block = held.at[slot, group]
        return remote(block, block, pass_sem.at[group, arrival], recv_sem.at[slot, group], (sibling, lane))

    part = seq % parts
    extent = shard_ref.shape[0] // parts
    mates = parts // 2
    first = chip // mates * mates

    def rows_of(index):
        return pl.ds(pl.multiple_of(index * extent, extent), extent)

    def wide(source, step):
        strip = wo.at[source, rows_of(part)]
        return remote(strip, strip, wide_send.at[step], wide_recv.at[source], (seq, (lane + step) % lanes))

    def mate(step):
        return first + (chip - first + step) % mates

    def spread(source, step):
        strip = wo.at[source, rows_of(part)]
        return remote(
            strip, strip, part_send.at[source, step], part_recv.at[source, part], (mate(step) * 2 + core, lane)
        )

    def share(source, index):
        strip = wo.at[source, rows_of(index)]
        return remote(strip, strip, part_pass.at[source, index], part_recv.at[source, index], (sibling, lane))

    def block(source, group, distance):
        rows_here = pl.ds(pl.multiple_of(group * width, width), width)
        strip = att.at[source, rows_here]
        return remote(
            strip, strip, block_send.at[distance + lanes, group], block_sem.at[source, group], (seq, lane + distance)
        )

    def inside(distance):
        return jnp.logical_and(lane + distance >= 0, lane + distance < lanes)

    def onward(group, action):
        for distance in range(2, lanes - 1):
            for sign in (1, -1):
                @when(inside(-sign * distance), inside(sign))
                def _():
                    copy = remote(
                        att.at[lane - sign * distance, pl.ds(pl.multiple_of(group * width, width), width)],
                        att.at[lane - sign * distance, pl.ds(pl.multiple_of(group * width, width), width)],
                        relay_send.at[sign * distance + lanes, group],
                        block_sem.at[lane - sign * distance, group],
                        (seq, lane + sign),
                    )
                    if action:
                        copy.wait_recv()
                        copy.start()
                    else:
                        copy.wait_send()

    barrier = pltpu.get_barrier_semaphore()
    pl.semaphore_signal(barrier, inc=1, device_id=(sibling, lane), device_id_type=MESH)
    for step in range(1, chips):
        pl.semaphore_signal(
            barrier, inc=1, device_id=(flip(chip, step, chips) * 2 + core, lane), device_id_type=MESH
        )
    for step in range(1, lanes):
        pl.semaphore_signal(barrier, inc=1, device_id=(seq, (lane + step) % lanes), device_id_type=MESH)

    own = pltpu.make_async_copy(qkv_ref, wq, load_sem.at[0])
    own.start()
    own_shard = pltpu.make_async_copy(shard_ref, wo.at[lane], load_sem.at[1])
    own_shard.start()
    loads = [
        pltpu.make_async_copy(up_ref, wu, load_sem.at[2]),
        pltpu.make_async_copy(down_ref, wd, load_sem.at[3]),
    ]
    for load in loads:
        load.start()
    normed = term

    @pl.loop(0, rows // sub)
    def _(index):
        span = pl.ds(pl.multiple_of(index * sub, sub), sub)
        normed[span, :] = layer_norm(tokens_ref[span, :].astype(jnp.float32), first_gain_ref[...]).astype(normed.dtype)

    pl.semaphore_wait(barrier, chips + lanes - 1)
    own_shard.wait()
    for step in range(1, lanes):
        wide(lane, step).start()
    own.wait()

    def project(which):
        return lax.dot_general(
            wq[which], normed[...], (((0,), (1,)), ((), ())), preferred_element_type=jnp.float32
        )

    for which in (1, 2):
        result = project(which).astype(jnp.bfloat16)
        for group in range(groups):
            strip = result[group * width : (group + 1) * width]
            held[seq, group, (which - 1) * size : which * size] = strip.reshape(size, HD, rows)

    def open_group(group):
        exchange(group, 0, 0).start()
        hand(group, 0, core).start()

    for group in range(groups):
        hand(group, 0, core).start()
    for group in range(min(2, groups)):
        exchange(group, 0, 0).start()
    query[...] = (project(0) * (LOG2E / HD**0.5)).astype(jnp.bfloat16).reshape(query.shape)

    def early(group):
        hand(group, 1, core).wait_recv()
        hand(group, 1, core).start()
        for stage in range(1, bits):
            exchange(group, 1, stage).start()

        @pl.when(group + 2 < groups)
        def _():
            exchange(group + 2, 0, 0).start()

        @pl.when(group + 1 < groups)
        def _():
            for stage in range(1, bits):
                exchange(group + 1, 0, stage).start()

    def prepare(group, index):
        arrival, second = index // 2, index % 2
        which = core + second - 2 * core * second

        @pl.when(index != 2)
        def _():
            hand(group, arrival, which).wait_recv()

        @when(second == 0, arrival > 1)
        def _():
            hand(group, arrival, core).start()
            for stage in range(2, bits):
                @pl.when(arrival < 2**stage)
                def _():
                    exchange(group, arrival, stage).start()

    def score(slot, group, member, target):
        result = lax.dot_general(
            held[slot, group, member], query[group * size + member], CONTRACT_FIRST,
            preferred_element_type=jnp.float32,
        )
        target[...] = result
        return jnp.max(result, axis=0, keepdims=True)

    def attend(slot, group, member, source, top):
        value = held[slot, group, size + member]
        head = group * size + member
        value = jnp.concatenate([value, jnp.ones((ONES, rows), value.dtype)], axis=0)
        old = peak[head]
        new = jnp.maximum(old, top)
        weights = jnp.exp2(source[...] - new).astype(jnp.bfloat16)
        term_here = jnp.dot(value, weights, preferred_element_type=jnp.float32)
        accum[head] = accum[head] * jnp.exp2(old - new) + term_here
        peak[head] = new

    scores = (score_a, score_b)
    column[...] = score(seq, 0, 0, score_a)

    accum[...] = jnp.zeros_like(accum)
    peak[...] = jnp.full_like(peak, -1e30)
    local, total_turns = 2 * groups, n * groups

    def locate(turn):
        later = turn - local
        group = jnp.where(turn < local, turn // 2, later // (n - 2))
        index = jnp.where(turn < local, turn % 2, 2 + later % (n - 2))
        arrival, second = index // 2, index % 2
        return group, index, slot_of(arrival, core + second - 2 * core * second)

    @pl.loop(0, total_turns)
    def _(turn):
        group, index, slot = locate(turn)

        @pl.when(turn == min(2, local - 1))
        def _():
            for stage in range(1, bits):
                exchange(0, 0, stage).start()

        @pl.when(turn == min(4, local - 1))
        def _():
            early(0)

        @when(index == 3, group + 1 < groups)
        def _():
            early(group + 1)

        @when(index == 4, group == max(groups - 2, 0))
        def _():
            for step in range(1, lanes):
                source = (lane + step) % lanes
                wide(source, step).wait_recv()
                share(source, part).start()
                for other in range(1, mates):
                    spread(source, other).start()

        next_group, next_index, next_slot = locate(jnp.minimum(turn + 1, total_turns - 1))

        @when(turn + 1 < total_turns, next_index > 0)
        def _():
            prepare(next_group, next_index)

        top = column[...]
        for member in range(size):
            if member < size - 1:
                below = score(slot, group, member + 1, scores[(member + 1) % 2])
            else:
                below = score(next_slot, next_group, 0, scores[(member + 1) % 2])
            attend(slot, group, member, scores[member % 2], top)
            top = below

        column[...] = top

        @pl.when(index == n - 1)
        def _():
            for member in range(size):
                head = group * size + member
                rows_here = pl.ds(pl.multiple_of(head * HD, HD), HD)
                att[lane, rows_here, :] = (accum[head, :HD] / accum[head, HD : HD + 1]).astype(att.dtype)
            for distance in (2, -2, 1, -1):
                @pl.when(inside(distance))
                def _():
                    block(lane, group, distance).start()

            @pl.when(group > 0)
            def _():
                onward(group - 1, True)

    onward(groups - 1, True)

    for step in range(1, lanes):
        source = (lane + step) % lanes
        for other in range(1, mates):
            index = (mate(other) * 2 + core) % parts
            share(source, index).wait_recv()
            share(source, index).start()
    for step in range(1, lanes):
        source = (lane + step) % lanes
        for other in range(mates):
            share(source, (mate(other) * 2 + 1 - core) % parts).wait_recv()
    for group in range(groups):
        for distance in (1, 2, *range(3, lanes)):
            for sign in (1, -1):
                if distance < 2 or distance == lanes - 1:
                    arrived = inside(sign * distance)
                else:
                    arrived = jnp.logical_and(inside(sign * distance), jnp.logical_not(inside(-sign)))

                @pl.when(arrived)
                def _():
                    block(lane + sign * distance, group, 1).wait_recv()
    for load in loads:
        load.wait()

    full, rest = rows // chunk, rows % chunk
    chunks, pieces = full + (rest > 0), rows // sub
    middle = lanes // 2
    on_left = lane < middle
    depth = jnp.where(on_left, lane, lanes - 1 - lane)
    inner = jnp.where(on_left, lane + 1, lane - 1)
    outer = jnp.where(on_left, lane - 1, lane + 1)
    central = depth == middle - 1

    def piece(index):
        return pl.ds(pl.multiple_of(index * sub, sub), sub)

    def inward(index, box):
        return remote(
            term.at[piece(index)], inbox.at[box, piece(index)],
            in_send.at[index], in_sem.at[box, index], (seq, inner),
        )

    def outward(index):
        return remote(
            res.at[piece(index)], res.at[piece(index)], out_send.at[index], out_sem.at[index], (seq, outer)
        )

    def store(index):
        return pltpu.make_async_copy(res.at[piece(index)], o_ref.at[piece(index)], store_sem.at[index])

    def compute(start, count):
        span = pl.ds(start, count)
        attended = att[:, :, span].reshape(-1, count)
        total = tokens_ref[span, :].astype(jnp.float32) + lax.dot_general(
            attended, wo[...].reshape(-1, wo.shape[2]), CONTRACT_FIRST, preferred_element_type=jnp.float32
        )
        mixed[span, :] = total
        post = layer_norm(total, gain_ref[...]).astype(jnp.bfloat16)
        hidden = jax.nn.gelu(
            jnp.dot(post, wu[...], preferred_element_type=jnp.float32), approximate=True
        ).astype(jnp.bfloat16)
        term[span, :] = jnp.dot(hidden, wd[...], preferred_element_type=jnp.float32).astype(jnp.bfloat16)

    def reduce_inward(index):
        @pl.when(depth > 0)
        def _():
            inward(index, 0).wait_recv()
            rows_here = piece(index)
            term[rows_here, :] = (
                term[rows_here, :].astype(jnp.float32) + inbox[0, rows_here, :].astype(jnp.float32)
            ).astype(jnp.bfloat16)

        inward(index, jnp.where(central, 1, 0)).start()

    def finish(index):
        inward(index, 1).wait_recv()
        rows_here = piece(index)
        both = term[rows_here, :].astype(jnp.float32) + inbox[1, rows_here, :].astype(jnp.float32)
        res[rows_here, :] = (mixed[rows_here, :] + both).astype(jnp.bfloat16)

        @pl.when(depth > 0)
        def _():
            outward(index).start()

        store(index).start()

    def relay(index):
        outward(index).wait_recv()

        @pl.when(depth > 0)
        def _():
            outward(index).start()

        store(index).start()

    lag = 2

    @pl.loop(0, chunks + middle - 1)
    def _(step):
        @pl.when(step < full)
        def _():
            compute(pl.multiple_of(step * chunk, chunk), chunk)

        if rest:
            @pl.when(step == full)
            def _():
                compute(full * chunk, rest)

        behind = step - depth

        @when(behind >= 0, behind < chunks)
        def _():
            @pl.loop(behind * chunk // sub, jnp.minimum(behind * chunk + chunk, rows) // sub)
            def _(index):
                reduce_inward(index)

                @when(central, index >= lag)
                def _():
                    finish(index - lag)

    @pl.when(central)
    def _():
        for index in range(pieces - lag, pieces):
            finish(index)

    @pl.when(jnp.logical_not(central))
    def _():
        @pl.loop(0, pieces)
        def _(index):
            relay(index)

    @pl.loop(0, groups)
    def _(group):
        for distance in (1, -1, 2, -2):
            @pl.when(inside(distance))
            def _():
                block(lane, group, distance).wait_send()

        onward(group, False)


        for arrival in range(chips):
            hand(group, arrival, core).wait_send()
            for stage in range(bits):
                if arrival < 2**stage:
                    exchange(group, arrival, stage).wait_send()

    for step in range(1, lanes):
        wide(lane, step).wait_send()
        source = (lane + step) % lanes
        share(source, part).wait_send()
        for other in range(1, mates):
            spread(source, other).wait_send()
            share(source, (mate(other) * 2 + core) % parts).wait_send()

    @pl.loop(0, pieces)
    def _(index):
        inward(index, 0).wait_send()
        store(index).wait()

        @pl.when(depth > 0)
        def _():
            outward(index).wait_send()


def fused(n, lanes, tokens, first_gain, w_qkv, gain, w_out, w_up, w_down):
    rows, width = tokens.shape
    span, hidden = w_out.shape[0], w_up.shape[1]
    heads = span // HD
    size = 2
    groups = heads // size
    parts = n
    while span // parts % 16 or span % parts:
        parts //= 2
    chips = n // 2
    bits = chips.bit_length() - 1
    chunk = 128
    sub = max(size for size in (16, 32, 48) if rows % size == 0)
    pieces = rows // sub
    vmem = pl.BlockSpec(memory_space=pltpu.VMEM)
    hbm = pl.BlockSpec(memory_space=pl.ANY)
    dma = pltpu.SemaphoreType.DMA
    return pl.pallas_call(
        functools.partial(layer_kernel, n, lanes, parts, chunk, sub, groups, size),
        out_shape=jax.ShapeDtypeStruct((rows, width), jnp.bfloat16),
        in_specs=[vmem, vmem, hbm, vmem, hbm, hbm, hbm],
        out_specs=hbm,
        scratch_shapes=[
            pltpu.VMEM((heads, HD, rows), jnp.bfloat16),
            pltpu.VMEM(w_qkv.shape, jnp.bfloat16),
            pltpu.VMEM((n, groups, 2 * size, HD, rows), jnp.bfloat16),
            pltpu.VMEM((rows, rows), jnp.float32),
            pltpu.VMEM((rows, rows), jnp.float32),
            pltpu.VMEM((1, rows), jnp.float32),
            pltpu.VMEM((heads, HD + ONES, rows), jnp.float32),
            pltpu.VMEM((heads, 1, rows), jnp.float32),
            pltpu.VMEM((lanes, span, rows), jnp.bfloat16),
            pltpu.VMEM((lanes, span, width), jnp.bfloat16),
            pltpu.VMEM((width, hidden), jnp.bfloat16),
            pltpu.VMEM((hidden, width), jnp.bfloat16),
            pltpu.VMEM((rows, width), jnp.float32),
            pltpu.VMEM((rows, width), jnp.bfloat16),
            pltpu.VMEM((2, rows, width), jnp.bfloat16),
            pltpu.VMEM((rows, width), jnp.bfloat16),
            dma((4,)),
            dma((n, groups)),
            dma((bits, groups, chips)),
            dma((groups, chips)),
            dma((lanes,)),
            dma((lanes,)),
            dma((lanes, parts // 2)),
            dma((lanes, parts)),
            dma((lanes, parts)),
            dma((lanes, groups)),
            dma((2 * lanes, groups)),
            dma((2 * lanes, groups)),
            dma((pieces,)),
            dma((2, pieces)),
            dma((pieces,)),
            dma((pieces,)),
            dma((pieces,)),
        ],
        compiler_params=pltpu.CompilerParams(
            collective_id=0, has_side_effects=True, vmem_limit_bytes=63 * 2**20
        ),
        cost_estimate=pl.CostEstimate(
            flops=4 * n * heads * rows * rows * HD + 2 * rows * width * (lanes * span + 2 * hidden),
            bytes_accessed=2 * width * (lanes * span + 2 * hidden),
            transcendentals=n * heads * rows * rows,
        ),
    )(tokens, first_gain, w_qkv, gain, w_out, w_up, w_down)


def per_device(n, lanes, tokens, norm_gain, w_qkv, w_out, post_gain, w_up, w_down):
    w_qkv = w_qkv.transpose(1, 0, 2)
    return fused(n, lanes, tokens, norm_gain, w_qkv, post_gain, w_out, w_up, w_down)


def solution(mesh):
    placed = (
        P("seq", None),
        P(),
        P(None, None, "tensor"),
        P("tensor", None),
        P(),
        P(None, "tensor"),
        P("tensor", None),
    )
    return jax.shard_map(
        functools.partial(per_device, mesh.shape["seq"], mesh.shape["tensor"]),
        mesh=mesh,
        in_specs=placed,
        out_specs=P("seq", None),
        check_vma=False,
    )
```
